8 devices in a mesh: data: 2 (over z, y), dap: 4 (over x, core).
Axes of the slice: x: 2, y: 2, z: 1, core: 2. Of those that a mesh axis runs over, the one named last changes fastest.
Arguments:
- z_one: bfloat16 [1024, 512, 128], P(('data', 'dap')), parts along dimension 0
- mask_one: int32 [1024, 512], P(('data', 'dap')), parts along dimension 0
- z_two: bfloat16 [1024, 512, 128], P(('data', 'dap')), parts along dimension 0
- mask_two: int32 [1024, 512], P(('data', 'dap')), parts along dimension 0
- norm_in: bfloat16 [2, 2, 128], replicated
- w_proj: bfloat16 [2, 128, 512], replicated
- w_gate: bfloat16 [2, 128, 128], replicated
- norm_mid: bfloat16 [2, 2, 128], replicated
- w_out: bfloat16 [2, 128, 128], replicated
Outputs:
- output 1: bfloat16 [1024, 512, 128], P(('data', 'dap')), parts along dimension 0
- output 2: bfloat16 [1024, 512, 128], P(('data', 'dap')), parts along dimension 0
There are 2 independent parts. The reference program is written for one: setup_inputs(seed, part) draws one part's arguments, and reference() takes and returns one part's arrays. A program takes and returns all parts, laid end to end along the dimension named above; an argument that names none is the same for every part.
All inputs are finite; a program needn't handle non-finite values.
Results may differ from the reference program's by a relative error of at most 0.00666387.
Values are sent between devices in bfloat16 or wider.
A program may use at most 1 GiB of HBM per device.

```python
import jax
import jax.numpy as jnp
from jax import lax

N = 512
CZ = 128
C = 128


def layer_norm(vals, ln_gain, ln_shift):
    vals = vals.astype(jnp.float32)
    row_mean = jnp.mean(vals, axis=-1, keepdims=True)
    centred = vals - row_mean
    row_var = jnp.mean(centred * centred, axis=-1, keepdims=True)
    return centred * lax.rsqrt(row_var + 1e-5) * ln_gain.astype(jnp.float32) + ln_shift.astype(jnp.float32)


def draw_mask(mask_key):
    residue_ok = (jax.random.randint(mask_key, (N,), 0, 20) != 0).astype(jnp.int32)
    return residue_ok[:, None] * residue_ok[None, :]


def setup_inputs(seed: int = 0, part: int = 0) -> dict:
    part_keys = jax.random.split(jax.random.fold_in(jax.random.key(seed), part), 4)
    shared_keys = jax.random.split(jax.random.key(seed + 1), 5)
    norm_base = jnp.array([1.0, 0.0], jnp.float32)[None, :, None]
    return {
        "z_one": jax.random.normal(part_keys[0], (N, N, CZ), jnp.float32).astype(jnp.bfloat16),
        "mask_one": draw_mask(part_keys[1]),
        "z_two": jax.random.normal(part_keys[2], (N, N, CZ), jnp.float32).astype(jnp.bfloat16),
        "mask_two": draw_mask(part_keys[3]),
        "norm_in": (0.3 * jax.random.normal(shared_keys[0], (2, 2, CZ), jnp.float32) + norm_base).astype(jnp.bfloat16),
        "w_proj": (jax.random.normal(shared_keys[1], (2, CZ, 4 * C), jnp.float32) * CZ ** -0.5).astype(jnp.bfloat16),
        "w_gate": (jax.random.normal(shared_keys[2], (2, CZ, CZ), jnp.float32) * CZ ** -0.5).astype(jnp.bfloat16),
        "norm_mid": (0.3 * jax.random.normal(shared_keys[3], (2, 2, C), jnp.float32) + norm_base).astype(jnp.bfloat16),
        "w_out": (jax.random.normal(shared_keys[4], (2, C, CZ), jnp.float32) * C ** -0.5).astype(jnp.bfloat16),
    }


def project_row(z_row, mask_row, norm_in, w_proj):
    x_row = layer_norm(z_row, norm_in[0], norm_in[1]).astype(jnp.bfloat16)
    projected = jnp.dot(x_row, w_proj, preferred_element_type=jnp.float32)
    keep_mask = mask_row.astype(jnp.float32)[:, None]
    a_row = keep_mask * jax.nn.sigmoid(projected[:, C:2 * C]) * projected[:, :C]
    b_row = keep_mask * jax.nn.sigmoid(projected[:, 3 * C:]) * projected[:, 2 * C:3 * C]
    return a_row.astype(jnp.bfloat16), b_row.astype(jnp.bfloat16)


def output_row(z_row, t_row, norm_in, w_gate, norm_mid, w_out):
    x_row = layer_norm(z_row, norm_in[0], norm_in[1]).astype(jnp.bfloat16)
    gate_val = jax.nn.sigmoid(jnp.dot(x_row, w_gate, preferred_element_type=jnp.float32))
    t_norm = layer_norm(t_row, norm_mid[0], norm_mid[1]).astype(jnp.bfloat16)
    update = jnp.dot(t_norm, w_out, preferred_element_type=jnp.float32)
    return (z_row.astype(jnp.float32) + gate_val * update).astype(jnp.bfloat16)


def tri_update(z_pair, pair_mask, norm_in, w_proj, w_gate, norm_mid, w_out, form):
    a_side, b_side = lax.map(lambda row_pair: project_row(row_pair[0], row_pair[1], norm_in, w_proj), (z_pair, pair_mask))
    tri_prod = jnp.einsum(form, a_side.astype(jnp.float32), b_side.astype(jnp.float32)).astype(jnp.bfloat16)
    return lax.map(lambda row_pair: output_row(row_pair[0], row_pair[1], norm_in, w_gate, norm_mid, w_out), (z_pair, tri_prod))


def run_crop(z_pair, pair_mask, norm_in, w_proj, w_gate, norm_mid, w_out):
    z_mid = tri_update(z_pair, pair_mask, norm_in[0], w_proj[0], w_gate[0], norm_mid[0], w_out[0], "ikc,jkc->ijc")
    return tri_update(z_mid, pair_mask, norm_in[1], w_proj[1], w_gate[1], norm_mid[1], w_out[1], "kic,kjc->ijc")


def reference(z_one, mask_one, z_two, mask_two, norm_in, w_proj, w_gate, norm_mid, w_out):
    return (run_crop(z_one, mask_one, norm_in, w_proj, w_gate, norm_mid, w_out),
            run_crop(z_two, mask_two, norm_in, w_proj, w_gate, norm_mid, w_out))
```

```python
import functools

import jax
import jax.numpy as jnp
from jax import lax
from jax.experimental import pallas as pl
from jax.experimental.pallas import tpu as pltpu
from jax.sharding import PartitionSpec as P


F32, BF16 = jnp.float32, jnp.bfloat16
ROWS, N, C = 128, 512, 128
RB = 16
UNROLL = 8
CG = 8
CHUNK = 32
ACROSS = [(0, 2), (2, 0), (1, 3), (3, 1)]
ON_CHIP = [(0, 1), (1, 0), (2, 3), (3, 2)]


def cost(us):
    return pl.CostEstimate(flops=int(us * 4e8), bytes_accessed=int(us * 2e6), transcendentals=0)


def ln_rows(v, gain, shift):
    cen = v - jnp.mean(v, axis=-1, keepdims=True)
    var = jnp.mean(cen * cen, axis=-1, keepdims=True)
    return (cen * lax.rsqrt(var + 1e-5) * gain + shift).astype(BF16)


def sigmoid(v):
    return 0.5 * jnp.tanh(0.5 * v) + 0.5


def dot_nt(a, b):
    return lax.dot_general(a, b, (((1,), (1,)), ((), ())), preferred_element_type=F32)


def dot_tn(a, b):
    return lax.dot_general(a, b, (((0,), (0,)), ((), ())), preferred_element_type=F32)


def cat(refs, c, axis=0):
    return refs[0][c] if len(refs) == 1 else jnp.concatenate([r[c] for r in refs], axis=axis)


def proj_body(z_ref, m_ref, n_ref, w_ref, scr):
    gain, shift = n_ref[0:1, :], n_ref[1:2, :]

    def row(i, carry):
        x = ln_rows(z_ref[i].astype(F32), gain, shift)
        keep = m_ref[i].astype(F32)
        for side in range(2):
            pg = dot_nt(w_ref[side * 256:(side + 1) * 256, :], x)
            scr[side, i] = (keep * sigmoid(pg[128:]) * pg[:128]).astype(BF16)
        return carry

    lax.fori_loop(0, RB, row, 0, unroll=UNROLL)


def proj_out_kernel(z_ref, m_ref, n_ref, w_ref, a_ref, b_ref, scr):
    proj_body(z_ref, m_ref, n_ref, w_ref, scr)
    a_ref[...] = jnp.transpose(scr[0], (1, 0, 2))
    b_ref[...] = jnp.transpose(scr[1], (1, 0, 2))


def proj_in_kernel(pos_ref, z_ref, m_ref, n_ref, w_ref, mine_ref, other_ref, b_ref, scr):
    proj_body(z_ref, m_ref, n_ref, w_ref, scr)
    for k in range(2):
        mine, other = (pl.multiple_of(pos_ref[2 * o + k] * ROWS, ROWS) for o in range(2))
        lanes = pl.ds(k * ROWS, ROWS)
        mine_ref[:, :, lanes] = jnp.transpose(scr[0, :, :, pl.ds(mine, ROWS)], (1, 0, 2))
        other_ref[:, :, lanes] = jnp.transpose(scr[0, :, :, pl.ds(other, ROWS)], (1, 0, 2))
    b_ref[...] = jnp.transpose(scr[1], (1, 0, 2))


def whole(shape):
    return pl.BlockSpec(shape, lambda r, *_: (0,) * len(shape))


def project(z, mask, norm, w_t, pos=None):
    rows = z.shape[0]
    slab = lambda lanes: pl.BlockSpec((C, RB, lanes), lambda r, *_: (0, r, 0))
    lanes = (N, N) if pos is None else (2 * ROWS, 2 * ROWS, N)
    grid_spec = pltpu.PrefetchScalarGridSpec(
        num_scalar_prefetch=0 if pos is None else 1, grid=(rows // RB,),
        in_specs=[pl.BlockSpec((RB, N, C), lambda r, *_: (r, 0, 0)), pl.BlockSpec((RB, 1, N), lambda r, *_: (r, 0, 0)),
                  whole((2, C)), whole((4 * C, C))],
        out_specs=[slab(w) for w in lanes],
        scratch_shapes=[pltpu.VMEM((2, RB, C, N), BF16)])
    args = (z, mask.reshape(rows, 1, N), norm, w_t)
    return pl.pallas_call(
        proj_out_kernel if pos is None else proj_in_kernel, grid_spec=grid_spec,
        out_shape=[jax.ShapeDtypeStruct((C, rows, w), BF16) for w in lanes],
        cost_estimate=cost(0.4 * rows))(*(args if pos is None else (pos,) + args))


def finish_kernel(t_ref, z_ref, n_ref, mid_ref, wg_ref, wo_ref, o_ref, scr):
    gain, shift = n_ref[0:1, :], n_ref[1:2, :]
    mid_gain, mid_shift = mid_ref[0], mid_ref[1]
    scr[...] = jnp.transpose(t_ref[...], (1, 0, 2))

    def row(i, carry):
        v = scr[i].astype(F32)
        cen = v - jnp.mean(v, axis=0, keepdims=True)
        var = jnp.mean(cen * cen, axis=0, keepdims=True)
        y = (cen * lax.rsqrt(var + 1e-5) * mid_gain + mid_shift).astype(BF16)
        update = dot_tn(y, wo_ref[...])
        z_row = z_ref[i].astype(F32)
        gate = sigmoid(jnp.dot(ln_rows(z_row, gain, shift), wg_ref[...], preferred_element_type=F32))
        o_ref[i] = (z_row + gate * update).astype(BF16)
        return carry

    lax.fori_loop(0, RB, row, 0, unroll=UNROLL)


def finish(t, z, norm, mid, w_gate, w_out, first=0, rows=ROWS):
    start = first // RB
    return pl.pallas_call(
        finish_kernel, grid=(rows // RB,), out_shape=jax.ShapeDtypeStruct((rows, N, C), BF16),
        in_specs=[pl.BlockSpec((C, RB, N), lambda r: (0, r + start, 0)), pl.BlockSpec((RB, N, C), lambda r: (r + start, 0, 0)),
                  whole((2, C)), whole((2, C, 1)), whole((C, C)), whole((C, C))],
        out_specs=pl.BlockSpec((RB, N, C), lambda r: (r, 0, 0)),
        scratch_shapes=[pltpu.VMEM((RB, C, N), BF16)], cost_estimate=cost(0.44 * rows))(t, z, norm, mid, w_gate, w_out)


def contract_out_kernel(counts, pos_ref, *refs):
    na, nb, nr = counts
    a_refs, b_refs, r_refs, (t0_ref, t1_ref) = refs[:na], refs[na:na + nb], refs[na + nb:na + nb + nr], refs[na + nb + nr:]
    for c in range(CG):
        a = cat(a_refs, c)
        for o, side in enumerate((b_refs, r_refs)):
            t = dot_nt(a, cat(side, c)).astype(BF16)
            for k in range(2):
                lanes = pl.ds(pl.multiple_of(pos_ref[2 * o + k] * ROWS, ROWS), ROWS)
                t0_ref[c, :, lanes] = t[:ROWS, k * ROWS:(k + 1) * ROWS]
                t1_ref[c, :, lanes] = t[ROWS:, k * ROWS:(k + 1) * ROWS]


def contract_out(pos, a, b, r):
    part = lambda v: pl.BlockSpec((CG,) + v.shape[1:], lambda g, *_: (g, 0, 0))
    ops = list(a) + list(b) + list(r)
    t = jax.ShapeDtypeStruct((C, ROWS, N), BF16)
    grid_spec = pltpu.PrefetchScalarGridSpec(num_scalar_prefetch=1, grid=(C // CG,), in_specs=[part(v) for v in ops],
                                             out_specs=[part(t)] * 2)
    return pl.pallas_call(functools.partial(contract_out_kernel, (len(a), len(b), len(r))), grid_spec=grid_spec,
                          out_shape=[t, t], cost_estimate=cost(50))(pos, *ops)


def contract_in_kernel(count, *refs):
    a_refs, b_refs, t_ref = refs[:count], refs[count:2 * count], refs[2 * count]
    for c in range(CG):
        t_ref[c] = dot_tn(cat(a_refs, c), cat(b_refs, c)).astype(BF16)


def contract_in(a, b, slot):
    t = jax.ShapeDtypeStruct((C, ROWS, N), BF16)
    return pl.pallas_call(
        functools.partial(contract_in_kernel, len(a)), grid=(C // CG,), out_shape=t,
        in_specs=[pl.BlockSpec((CG, v.shape[1], ROWS), lambda g: (g, 0, slot)) for v in a]
        + [pl.BlockSpec((CG, v.shape[1], N), lambda g: (g, 0, 0)) for v in b],
        out_specs=pl.BlockSpec((CG, ROWS, N), lambda g: (g, 0, 0)), cost_estimate=cost(30))(*a, *b)


def solution(mesh):
    row_spec, mask_spec, replicated = P(("data", "dap"), None, None), P(("data", "dap"), None), P()

    def across(v):
        return lax.ppermute(v, "dap", ACROSS)

    def on_chip(v):
        return lax.ppermute(v, "dap", ON_CHIP)

    def update_crops(z_one, mask_one, z_two, mask_two, norm_in, w_proj, w_gate, norm_mid, w_out):
        me = lax.axis_index("dap")
        chip, core = me // 2, me % 2
        first = chip == 0
        pos = jnp.stack([2 * chip + core, 2 * (1 - chip) + core, 2 * chip + 1 - core, 2 * (1 - chip) + 1 - core]).astype(jnp.int32)
        norm_in, norm_mid = norm_in.astype(F32), norm_mid.astype(F32)[..., None]
        w_t = jnp.swapaxes(w_proj, 1, 2)

        pieces = [slice(r, r + CHUNK) for r in range(0, ROWS, CHUNK)]
        mask_got = across(jnp.where(first, mask_two, mask_one))
        z_got = []
        for p in pieces:
            z_got.append(across(jnp.where(first, z_two[p], z_one[p])))
        z_own = jnp.where(first, z_one, z_two)
        mask_own = jnp.where(first, mask_one, mask_two)

        a_own, b_own = project(z_own, mask_own, norm_in[0], w_t[0])
        a, b = map(list, zip((a_own, b_own), *(project(z, mask_got[p], norm_in[0], w_t[0]) for z, p in zip(z_got, pieces))))
        t = contract_out(pos, a, b, [on_chip(v) for v in b])
        z_got = jnp.concatenate(z_got, axis=0)
        z_mid = [finish(t[s], z, norm_in[0], norm_mid[0], w_gate[0], w_out[0]) for s, z in enumerate((z_own, z_got))]

        mine, other, b = map(list, zip(*(project(z_mid[s], m, norm_in[1], w_t[1], pos) for s, m in enumerate((mask_own, mask_got)))))
        a = mine + [on_chip(v) for v in other]
        b = b + [on_chip(v) for v in b]
        t_back = contract_in(a, b, 1)
        back = [across(finish(t_back, z_mid[1], norm_in[1], norm_mid[1], w_gate[1], w_out[1], p.start, CHUNK)) for p in pieces]
        own = finish(contract_in(a, b, 0), z_mid[0], norm_in[1], norm_mid[1], w_gate[1], w_out[1])
        back = jnp.concatenate(back, axis=0)
        return jnp.where(first, own, back), jnp.where(first, back, own)

    return jax.shard_map(update_crops, mesh=mesh,
                         in_specs=(row_spec, mask_spec, row_spec, mask_spec) + (replicated,) * 5,
                         out_specs=(row_spec, row_spec), check_vma=False)
```
